1024 devices in a mesh: gx: 16 (over x, core), gy: 8 (over y), gz: 8 (over z).
Axes of the slice: x: 8, y: 8, z: 8, core: 2. Of those that a mesh axis runs over, the one named last changes fastest.
Arguments:
- local_schur: float32 [1024, 1024], replicated, may hold values from -1 to 4, as said below
- block_inverse: float32 [1024, 1024], replicated, may hold values from -1 to 1, as said below
- coefficient: float32 [16, 8, 8], P('gx', 'gy', 'gz'), may hold values from 0.3 to 3
- face_index: int32 [1024], replicated, may hold values from 0 to 1023, each once
- right_side: float32 [16, 8, 8, 1024, 128], P('gx', 'gy', 'gz'), may hold values from -6 to 6
Outputs:
- solution: float32 [16, 8, 8, 1024, 128], P('gx', 'gy', 'gz')
- residual: float32 [16, 8, 8, 1024, 128], P('gx', 'gy', 'gz')
The draws below stay inside these ranges and needn't reach their ends.
Inputs may be any that keep to these rules, and one draw needn't show every extreme that they name: `local_schur`: symmetric positive definite. `block_inverse`: symmetric positive definite. `face_index`: entries k * 128 to (k + 1) * 128 - 1 list face k's unknowns as in the reference program; the last 256 entries are unknowns of one subdomain alone.
All inputs are finite; a program needn't handle non-finite values.
Results may differ from the reference program's by a relative error of at most 0.00022.
Values sent between devices are 32-bit elements; how exact they have to be, the bound alone decides.
No kernel may reach another device: no remote copies, remote signals or barrier semaphores. Data moves between devices by JAX's collectives and lax.ppermute only.
A program may use at most 32 MiB of HBM per device.

```python
import math
import jax
import jax.numpy as jnp
from jax import lax

W = 1024
FACE = 128
R = 128
PX = 16
PY = 8
PZ = 8


def symmetric_block(key, spread, low, high):
    first, second = jax.random.split(key)
    noise = jax.random.normal(first, (W, W), jnp.float32) * (spread / math.sqrt(W))
    diagonal = jax.random.uniform(second, (W,), jnp.float32, low, high)
    return noise + noise.T + jnp.diag(diagonal)


def draw_local_schur(key, part):
    return symmetric_block(jax.random.fold_in(key, 11), 0.32, 1.5, 3.0)


def draw_block_inverse(key, part):
    return symmetric_block(jax.random.fold_in(key, 23), 0.07, 0.3, 0.7)


def block_scale(rng, shape, cuts, low, top_value):
    def one(dim, parts):
        heights = jax.random.uniform(jax.random.fold_in(jax.random.fold_in(rng, 6), dim), (parts,), jnp.float32, low / len(cuts), top_value / len(cuts))
        return jnp.repeat(jnp.exp(heights), shape[dim] // parts).reshape((-1,) + (1,) * (len(shape) - dim - 1))

    level = one(*cuts[0])
    for cut in cuts[1:]:
        level = level * one(*cut)
    return level


def scatter_about(own_key, shape, scale, most, pieces=(), kind=jnp.bfloat16):
    values = jax.random.normal(own_key, shape, jnp.float32) * scale
    if len(pieces) > 0:
        values = block_scale(own_key, shape, pieces, -0.22, 0.18) * values
    return jnp.clip(values, min=-most, max=most).astype(kind)


def setup_inputs(seed: int = 0) -> dict:
    key_of = jax.random.split(jax.random.key(seed), 6)
    local_schur = draw_local_schur(jax.random.fold_in(key_of[5], 71), 0)
    block_inverse = draw_block_inverse(jax.random.fold_in(key_of[5], 71), 0)
    coefficient = jnp.clip(jnp.exp(math.log(3.0) - 2.3025851 * jax.random.uniform(key_of[2], (PX, PY, PZ), jnp.float32) ** block_scale(key_of[2], (PX, PY, PZ), ((0, 16), (1, 8), (2, 8)), -0.2, 0.2)), 0.3, 3.0)
    face_index = jax.random.permutation(key_of[3], W).astype(jnp.int32)
    right_side = scatter_about(key_of[4], (PX, PY, PZ, W, R), 1.0, 6.0, ((0, 16), (1, 8), (2, 8)), jnp.float32)
    return {"local_schur": local_schur, "block_inverse": block_inverse, "coefficient": coefficient, "face_index": face_index, "right_side": right_side}


def shift_down(arr, axis):
    pad = [(0, 0)] * arr.ndim
    pad[axis] = (1, 0)
    padded = jnp.pad(arr, pad)
    return lax.slice_in_dim(padded, 0, arr.shape[axis], axis=axis)


def shift_up(arr, axis):
    pad = [(0, 0)] * arr.ndim
    pad[axis] = (0, 1)
    padded = jnp.pad(arr, pad)
    return lax.slice_in_dim(padded, 1, arr.shape[axis] + 1, axis=axis)


def assemble(vec, flat_index):
    faces = vec[:, :, :, flat_index, :].reshape(PX, PY, PZ, 6, FACE, vec.shape[-1])
    adds = []
    for axis in range(3):
        minus = faces[:, :, :, 2 * axis]
        plus = faces[:, :, :, 2 * axis + 1]
        adds.append(shift_down(plus, axis))
        adds.append(shift_up(minus, axis))
    stacked = jnp.stack(adds, axis=3).reshape(PX, PY, PZ, 6 * FACE, vec.shape[-1])
    return vec.at[:, :, :, flat_index, :].add(stacked)


def make_weight(face_rows):
    weight = jnp.ones((PX, PY, PZ, W), jnp.float32)
    counts = (PX, PY, PZ)
    for axis in range(3):
        position = lax.broadcasted_iota(jnp.int32, (PX, PY, PZ, 1), axis)
        lower = jnp.where(position > 0, 0.5, 1.0).astype(jnp.float32)
        upper = jnp.where(position < counts[axis] - 1, 0.5, 1.0).astype(jnp.float32)
        weight = weight.at[:, :, :, face_rows[2 * axis]].set(jnp.broadcast_to(lower, (PX, PY, PZ, FACE)))
        weight = weight.at[:, :, :, face_rows[2 * axis + 1]].set(jnp.broadcast_to(upper, (PX, PY, PZ, FACE)))
    return weight


def reference(local_schur, block_inverse, coefficient, face_index, right_side):
    face_rows = face_index[:6 * FACE].reshape(6, FACE)
    flat_index = face_rows.reshape(-1)
    weight = make_weight(face_rows)[..., None]
    scale = coefficient[..., None, None]

    def product(matrix, vec):
        return jnp.einsum('ij,abcjr->abcir', matrix, vec, precision=lax.Precision.HIGHEST)

    def apply_operator(vec):
        return assemble(product(local_schur, vec) * scale, flat_index)

    def apply_precond(vec):
        return assemble(product(block_inverse, vec) / scale, flat_index)

    def dot(left, right):
        return jnp.sum(weight * left * right, axis=(0, 1, 2, 3))

    rhs = assemble(right_side, flat_index)
    solution = jnp.zeros_like(rhs)
    residual = rhs
    precond = apply_precond(residual)
    norm_now = dot(residual, precond)
    direction = precond
    for step in range(2):
        image = apply_operator(direction)
        alpha = norm_now / dot(direction, image)
        solution = solution + alpha * direction
        residual = residual - alpha * image
        if step == 0:
            precond = apply_precond(residual)
            norm_next = dot(residual, precond)
            direction = precond + (norm_next / norm_now) * direction
            norm_now = norm_next
    return solution, residual
```

```python
import functools

import jax
import jax.numpy as jnp
from jax import lax
from jax.experimental import pallas as pl
from jax.experimental.pallas import tpu as pltpu
from jax.sharding import Mesh
from jax.sharding import PartitionSpec as P

AXES = ("gx", "gy", "zh", "zl")
GZ = ("zh", "zl")
FIRST = ("gy", "zh")
SECOND = ("gx", "zl")
BLOCKS = 4
SLOTS = 16
VMEM = pl.BlockSpec(memory_space=pltpu.VMEM)
SMEM = pl.BlockSpec(memory_space=pltpu.SMEM)
HBM = pl.BlockSpec(memory_space=pltpu.HBM)


def params(mebibytes):
    return pltpu.CompilerParams(vmem_limit_bytes=mebibytes * 1024 * 1024)


def halves(value):
    high = value.astype(jnp.bfloat16)
    low = (value - high.astype(jnp.float32)).astype(jnp.bfloat16)
    return high, low


def side_by_side(value):
    return jnp.concatenate(halves(value), axis=1)


def dot(left, right):
    return jnp.dot(left, right, preferred_element_type=jnp.float32)


def folded(wide):
    columns = wide.shape[1] // 2
    return wide[:, :columns] + wide[:, columns:]


def pick_kernel(scalar_ref, row_ref, column_ref, rhs_ref, pick_ref, line_ref, own_ref, *face_refs):
    line_ref[...] = row_ref[...]
    own_ref[...] = rhs_ref[...]
    count, width = pick_ref.shape
    lanes = column_ref.shape[1]
    column = column_ref[...]
    lane = lax.broadcasted_iota(jnp.int32, (count, lanes), 1)
    for start in range(0, width, lanes):
        pick_ref[:, start : start + lanes] = jnp.where(column == lane + start, 1.0, 0.0).astype(
            jnp.bfloat16
        )
    faces = folded(dot(pick_ref[...], side_by_side(rhs_ref[...])))
    face = count // 6
    for k, ref in enumerate(face_refs):
        ref[...] = faces[k * face : (k + 1) * face]


def spread_kernel(row_ref, spread_ref):
    width, count = spread_ref.shape
    step = 128
    row = row_ref[...]
    for start in range(0, width, step):
        index = lax.broadcasted_iota(jnp.int32, (step, count), 0) + start
        spread_ref[start : start + step, :] = jnp.where(index == row, 1.0, 0.0).astype(jnp.bfloat16)


def added(local_ref, spread_ref, mask_ref, halo_refs):
    halo = jnp.concatenate(
        [jnp.where(mask_ref[k] > 0.0, ref[...], 0.0) for k, ref in enumerate(halo_refs)], axis=0
    )
    return local_ref[...] + folded(dot(spread_ref[...], side_by_side(halo)))


def apply_kernel(which, slot, scalar_ref, matrix_ref, pick_ref, spread_ref, local_ref, *refs):
    halo_refs = refs[:6]
    earlier = len(refs) - 18
    earlier_refs = refs[6 : 6 + earlier]
    store_ref, next_ref, sum_ref = refs[6 + earlier : 9 + earlier]
    face_refs = refs[9 + earlier : 15 + earlier]
    held_ref, kept_ref, sem_ref = refs[15 + earlier :]
    share = slot == 3
    if slot > 0:
        earlier_refs = earlier_refs[:-1]
    width = local_ref.shape[0]
    rows = width // BLOCKS

    def part(block):
        return pl.ds(block * rows, rows)

    def copy(block):
        return pltpu.make_async_copy(
            matrix_ref.at[part(block)], held_ref.at[part(block)], sem_ref.at[block]
        )

    for block in range(BLOCKS):
        copy(block).start()
    whole = added(local_ref, spread_ref, scalar_ref, halo_refs)
    kept_ref[...] = whole
    keep = pltpu.make_async_copy(kept_ref, store_ref.at[slot], sem_ref.at[BLOCKS])
    keep.start()
    sides = side_by_side(whole)
    scale = scalar_ref[which]
    total = jnp.zeros((1, whole.shape[1]), jnp.float32)
    for block in range(BLOCKS):
        copy(block).wait()
        high, low = halves(held_ref[block * rows : (block + 1) * rows, :])
        made = folded(dot(high, sides) + dot(low, sides)) * scale
        next_ref[block * rows : (block + 1) * rows, :] = made
        total = total + jnp.sum(
            made * whole[block * rows : (block + 1) * rows, :], axis=0, keepdims=True
        )
    if share:
        sums = jnp.concatenate([*(ref[...] for ref in earlier_refs), total], axis=0)
        sum_ref[...] = jnp.broadcast_to(sums[None], sum_ref.shape)
    else:
        sum_ref[...] = total
    faces = folded(dot(pick_ref[...], side_by_side(next_ref[...])))
    face = faces.shape[0] // 6
    for k, ref in enumerate(face_refs):
        ref[...] = faces[k * face : (k + 1) * face]
    keep.wait()


def relay_kernel(from_ref, to_ref):
    to_ref[...] = jnp.broadcast_to(jnp.sum(from_ref[...], axis=0, keepdims=True), to_ref.shape)


def last_kernel(scalar_ref, sums_ref, spread_ref, local_ref, *refs):
    halo_refs = refs[:6]
    store_ref, solution_ref, residual_ref, *held_refs, sem_ref = refs[6:]
    rhs_ref, z0_ref, w0_ref, z1_ref = held_refs
    copies = [
        pltpu.make_async_copy(store_ref.at[k], held, sem_ref.at[k])
        for k, held in enumerate(held_refs)
    ]
    for copy in copies:
        copy.start()
    last = added(local_ref, spread_ref, scalar_ref, halo_refs)
    sums = jnp.sum(sums_ref[...], axis=0)
    g1, g2, g3, g4 = (sums[k : k + 1] for k in range(4))
    first = g1 / g2
    ratio = g3 / g2
    second = (g2 - first * g3) / (g4 - ratio * g3)
    first = first - second * ratio
    for copy in copies:
        copy.wait()
    solution_ref[...] = first * z0_ref[...] + second * z1_ref[...]
    residual_ref[...] = rhs_ref[...] - first * w0_ref[...] - second * last


def exchange(faces):
    halo = [None] * 6
    order = (("gy", 2, 1), (GZ, 4, 1), ("gx", 0, 1), ("gy", 3, -1), (GZ, 5, -1), ("gx", 1, -1))
    for axis, target, way in order:
        count = lax.axis_size(axis)
        pairs = [(i, (i + way) % count) for i in range(count)]
        halo[target] = lax.ppermute(faces[target ^ 1], axis, pairs)
    return halo


def on_device(local_schur, block_inverse, coefficient, face_index, right_side):
    width = local_schur.shape[0]
    face = width // 8
    columns = right_side.shape[-1]
    count = 6 * face
    f32, bf16 = jnp.float32, jnp.bfloat16
    scale = coefficient.reshape(())
    rhs = right_side.reshape(width, columns)
    listed = face_index[:count]
    column = jnp.broadcast_to(listed[:, None], (count, 128))
    row = listed[None, :]
    masks = []
    for axis in ("gx", "gy", GZ):
        at = lax.axis_index(axis)
        masks += [at > 0, at < lax.axis_size(axis) - 1]
    masks = [mask.astype(f32) for mask in masks]
    scalars = jnp.stack([*masks, 1.0 / scale, scale])

    vector = jax.ShapeDtypeStruct((width, columns), f32)
    faces_out = [jax.ShapeDtypeStruct((face, columns), f32)] * 6
    line = jax.ShapeDtypeStruct((1, columns), f32)
    groups = (lax.axis_size(FIRST), lax.axis_size(SECOND))
    shared = [jax.ShapeDtypeStruct((group, 4, columns), f32) for group in groups]

    pick, row, local, *faces = pl.pallas_call(
        pick_kernel,
        out_shape=[
            jax.ShapeDtypeStruct((count, width), bf16),
            jax.ShapeDtypeStruct(row.shape, row.dtype),
            vector,
            *faces_out,
        ],
        in_specs=[SMEM] + [VMEM] * 3,
        out_specs=[VMEM] * 9,
        compiler_params=params(16),
        name="pick",
    )(scalars, row, column, rhs)
    halo = exchange(faces)
    spread = pl.pallas_call(
        spread_kernel,
        out_shape=jax.ShapeDtypeStruct((width, count), bf16),
        in_specs=[VMEM],
        out_specs=VMEM,
        compiler_params=params(16),
        cost_estimate=pl.CostEstimate(flops=2000000, bytes_accessed=0, transcendentals=0),
        name="spread",
    )(row)

    def apply_call(slot, matrix, local, halo, sums=(), stores=()):
        store, local, total, *faces = pl.pallas_call(
            functools.partial(apply_kernel, 6 + slot % 2, slot),
            out_shape=[
                jax.ShapeDtypeStruct((SLOTS, width, columns), f32),
                vector,
                shared[0] if sums else line,
                *faces_out,
            ],
            in_specs=[SMEM, HBM] + [VMEM] * (9 + len(sums)) + [HBM] * len(stores),
            out_specs=[HBM] + [VMEM] * 8,
            input_output_aliases={11 + len(sums): 0} if stores else {},
            scratch_shapes=[
                pltpu.VMEM((width, width), f32),
                pltpu.VMEM((width, columns), f32),
                pltpu.SemaphoreType.DMA((BLOCKS + 1,)),
            ],
            compiler_params=params(48),
            name="apply",
        )(scalars, matrix, pick, spread, local, *halo, *sums, *stores)
        return store, local, total, faces

    store, local, g1, faces = apply_call(0, block_inverse, local, halo)
    halo = exchange(faces)
    store, local, g2, faces = apply_call(1, local_schur, local, halo, (), (store,))
    halo = exchange(faces)
    store, local, g3, faces = apply_call(2, block_inverse, local, halo, (), (store,))
    halo = exchange(faces)
    store, local, sums, faces = apply_call(
        3, local_schur, local, halo, (g1, g2, g3), (store,)
    )
    sums = lax.all_to_all(sums, FIRST, 0, 0)
    sums = pl.pallas_call(
        relay_kernel,
        out_shape=shared[1],
        in_specs=[VMEM],
        out_specs=VMEM,
        compiler_params=params(16),
        name="relay",
    )(sums)
    sums = lax.all_to_all(sums, SECOND, 0, 0)
    halo = exchange(faces)
    solution, residual = pl.pallas_call(
        last_kernel,
        out_shape=[vector, vector],
        in_specs=[SMEM] + [VMEM] * 9 + [HBM],
        out_specs=[VMEM] * 2,
        scratch_shapes=[pltpu.VMEM((width, columns), f32)] * 4 + [pltpu.SemaphoreType.DMA((4,))],
        compiler_params=params(48),
        name="last",
    )(scalars, sums, spread, local, *halo, store)
    return (solution.reshape(1, 1, 1, width, columns), residual.reshape(1, 1, 1, width, columns))


def solution(mesh):
    gx, gy, gz = (mesh.shape[name] for name in ("gx", "gy", "gz"))
    split = Mesh(mesh.devices.reshape(gx, gy, gz // 2, 2), AXES)
    subdomain = P("gx", "gy", GZ)
    vectors = P("gx", "gy", GZ, None, None)
    return jax.shard_map(
        on_device,
        mesh=split,
        in_specs=(P(), P(), subdomain, P(), vectors),
        out_specs=(vectors, vectors),
        check_vma=False,
    )
```

```python
import functools

import jax
import jax.numpy as jnp
from jax import lax
from jax.experimental import pallas as pl
from jax.experimental.pallas import tpu as pltpu
from jax.sharding import Mesh
from jax.sharding import PartitionSpec as P

AXES = ("gx", "gy", "zh", "zl")
GZ = ("zh", "zl")
FIRST = ("gy", "zh")
SECOND = ("gx", "zl")
BLOCKS = 4
SLOTS = 16
LANES = 128
LATER = 40
VMEM = pl.BlockSpec(memory_space=pltpu.VMEM)
SMEM = pl.BlockSpec(memory_space=pltpu.SMEM)
HBM = pl.BlockSpec(memory_space=pltpu.HBM)


def params(mebibytes):
    return pltpu.CompilerParams(vmem_limit_bytes=mebibytes * 1024 * 1024)


def halves(value):
    high = value.astype(jnp.bfloat16)
    low = (value - high.astype(jnp.float32)).astype(jnp.bfloat16)
    return high, low


def side_by_side(value):
    return jnp.concatenate(halves(value), axis=1)


def dot(left, right):
    return jnp.dot(left, right, preferred_element_type=jnp.float32)


def folded(wide):
    columns = wide.shape[1] // 2
    return wide[:, :columns] + wide[:, columns:]


def pick_kernel(scalar_ref, index_ref, rhs_ref, pick_ref, line_ref, own_ref, *face_refs):
    count, width = pick_ref.shape
    line_ref[...] = index_ref[...]
    own = rhs_ref[...]
    own_ref[...] = own
    sides = side_by_side(own)
    lane = lax.broadcasted_iota(jnp.int32, (LANES, LANES), 1).astype(jnp.float32)
    lines = index_ref[...].astype(jnp.float32)
    for turn in range(count // LANES):
        line = jnp.broadcast_to(lines[turn : turn + 1, :], (LANES, LANES))
        listed = jnp.transpose(line)
        for start in range(0, width, LANES):
            pick_ref[turn * LANES : (turn + 1) * LANES, start : start + LANES] = jnp.where(
                listed == lane + float(start), 1.0, 0.0
            ).astype(jnp.bfloat16)
    put_faces(folded(dot(pick_ref[...], sides)), face_refs)


def spread_kernel(index_ref, spread_ref):
    width, count = spread_ref.shape
    lines = [index_ref[k : k + 1, :] for k in range(count // LANES)]
    place = lax.broadcasted_iota(jnp.int32, (LANES, LANES), 0)

    def step(turn, carry):
        rows = pl.ds(pl.multiple_of(turn * LANES, LANES), LANES)
        for k, line in enumerate(lines):
            spread_ref[rows, k * LANES : (k + 1) * LANES] = jnp.where(
                place + turn * LANES == line, 1.0, 0.0
            ).astype(jnp.bfloat16)
        return carry

    lax.fori_loop(0, width // LANES, step, 0)


def put_faces(found, face_refs):
    face = found.shape[0] // 6
    for k, ref in enumerate(face_refs):
        ref[...] = found[k * face : (k + 1) * face, :]


def taken(scalar_ref, halo_refs):
    faces = [jnp.where(scalar_ref[k] > 0.5, ref[...], 0.0) for k, ref in enumerate(halo_refs)]
    return side_by_side(jnp.concatenate(faces, axis=0))


def rows_of(block, rows):
    return pl.ds(pl.multiple_of(block * rows, rows), rows)


def apply_kernel(which, slot, scalar_ref, matrix_ref, pick_ref, spread_ref, local_ref, *refs):
    halo_refs = refs[:6]
    earlier = len(refs) - 19 - (slot == 0)
    earlier_refs = refs[6 : 6 + earlier]
    store_ref, next_ref, sum_ref = refs[6 + earlier : 9 + earlier]
    face_refs = refs[9 + earlier : 15 + earlier]
    kept_ref, sides_ref, found_ref, sem_ref, *held_refs = refs[15 + earlier :]
    share = slot == 3
    if slot > 0:
        earlier_refs = earlier_refs[:-1]
    width, columns = local_ref.shape
    rows = width // BLOCKS

    def copy(block):
        part = rows_of(block, rows)
        return pltpu.make_async_copy(
            matrix_ref.at[part], held_refs[0].at[part], sem_ref.at[block]
        )

    source_ref = matrix_ref
    if slot == 0:
        source_ref = held_refs[0]
        for block in range(BLOCKS):
            copy(block).start()
    halo = taken(scalar_ref, halo_refs)

    def add(block, carry):
        part = rows_of(block, rows)
        whole = local_ref[part, :] + folded(dot(spread_ref[part, :], halo))
        kept_ref[part, :] = whole
        high, low = halves(whole)
        sides_ref[part, :columns] = high
        sides_ref[part, columns:] = low
        return carry

    lax.fori_loop(0, BLOCKS, add, 0)
    keep = pltpu.make_async_copy(kept_ref, store_ref.at[slot], sem_ref.at[BLOCKS])
    keep.start()
    scale = scalar_ref[which]

    def multiply(block, total):
        part = rows_of(block, rows)
        if slot == 0:
            copy(block).wait()
        high, low = halves(source_ref[part, :])
        sides = sides_ref[...]
        made = folded(dot(high, sides) + dot(low, sides)) * scale
        next_ref[part, :] = made
        return total + jnp.sum(made * kept_ref[part, :], axis=0, keepdims=True)

    total = lax.fori_loop(0, BLOCKS, multiply, jnp.zeros((1, columns), jnp.float32))
    if share:
        sums = jnp.concatenate([*(ref[...] for ref in earlier_refs), total], axis=0)
        sum_ref[...] = jnp.broadcast_to(sums[None], sum_ref.shape)
    else:
        sum_ref[...] = total

    def split(block, carry):
        part = rows_of(block, rows)
        high, low = halves(next_ref[part, :])
        sides_ref[part, :columns] = high
        sides_ref[part, columns:] = low
        return carry

    lax.fori_loop(0, BLOCKS, split, 0)
    each = found_ref.shape[0] // 3

    def find(block, carry):
        part = rows_of(block, each)
        found_ref[part, :] = folded(dot(pick_ref[part, :], sides_ref[...]))
        return carry

    lax.fori_loop(0, 3, find, 0)
    put_faces(found_ref, face_refs)
    keep.wait()


def relay_kernel(from_ref, to_ref):
    to_ref[...] = jnp.broadcast_to(jnp.sum(from_ref[...], axis=0, keepdims=True), to_ref.shape)


def last_kernel(scalar_ref, sums_ref, spread_ref, local_ref, *refs):
    halo_refs = refs[:6]
    store_ref, solution_ref, residual_ref, *held_refs, sem_ref = refs[6:]
    rhs_ref, z0_ref, w0_ref, z1_ref = held_refs
    copies = [
        pltpu.make_async_copy(store_ref.at[k], held, sem_ref.at[k])
        for k, held in enumerate(held_refs)
    ]
    for copy in copies:
        copy.start()
    halo = taken(scalar_ref, halo_refs)
    sums = jnp.sum(sums_ref[...], axis=0)
    g1, g2, g3, g4 = (sums[k : k + 1] for k in range(4))
    first = g1 / g2
    ratio = g3 / g2
    second = (g2 - first * g3) / (g4 - ratio * g3)
    first = first - second * ratio
    last = local_ref[...] + folded(dot(spread_ref[...], halo))
    for copy in copies:
        copy.wait()
    solution_ref[...] = first * z0_ref[...] + second * z1_ref[...]
    residual_ref[...] = rhs_ref[...] - first * w0_ref[...] - second * last


def exchange(faces, order):
    halo = [None] * 6
    for target in order:
        axis = ("gx", "gy", GZ)[target // 2]
        way = 1 if target % 2 == 0 else -1
        count = lax.axis_size(axis)
        pairs = [(i, (i + way) % count) for i in range(count)]
        halo[target] = lax.ppermute(faces[target ^ 1], axis, pairs)
    return halo


def on_device(local_schur, block_inverse, coefficient, face_index, right_side):
    width = local_schur.shape[0]
    face = width // 8
    columns = right_side.shape[-1]
    count = 6 * face
    f32, bf16 = jnp.float32, jnp.bfloat16
    scale = coefficient.reshape(())
    rhs = right_side.reshape(width, columns)
    index = face_index.reshape(width // LANES, LANES)
    masks = []
    for axis in ("gx", "gy", GZ):
        at = lax.axis_index(axis)
        masks += [at > 0, at < lax.axis_size(axis) - 1]
    masks = [mask.astype(f32) for mask in masks]
    scalars = jnp.stack([*masks, 1.0 / scale, scale])

    vector = jax.ShapeDtypeStruct((width, columns), f32)
    faces_out = [jax.ShapeDtypeStruct((face, columns), f32)] * 6
    line = jax.ShapeDtypeStruct((1, columns), f32)
    groups = (lax.axis_size(FIRST), lax.axis_size(SECOND))
    shared = [jax.ShapeDtypeStruct((group, 4, columns), f32) for group in groups]

    pick, index, local, *faces = pl.pallas_call(
        pick_kernel,
        out_shape=[
            jax.ShapeDtypeStruct((count, width), bf16),
            jax.ShapeDtypeStruct(index.shape, index.dtype),
            vector,
            *faces_out,
        ],
        in_specs=[SMEM] + [VMEM] * 2,
        out_specs=[VMEM] * 9,
        compiler_params=params(16),
        name="pick",
    )(scalars, index, rhs)
    halo = exchange(faces, (4, 0, 5, 2, 3, 1))
    spread = pl.pallas_call(
        spread_kernel,
        out_shape=jax.ShapeDtypeStruct((width, count), bf16),
        in_specs=[VMEM],
        out_specs=VMEM,
        compiler_params=params(16),
        cost_estimate=pl.CostEstimate(flops=2000000, bytes_accessed=0, transcendentals=0),
        name="spread",
    )(index)

    def apply_call(slot, matrix, local, halo, sums=(), stores=()):
        store, local, total, *faces = pl.pallas_call(
            functools.partial(apply_kernel, 6 + slot % 2, slot),
            out_shape=[
                jax.ShapeDtypeStruct((SLOTS, width, columns), f32),
                vector,
                shared[0] if sums else line,
                *faces_out,
            ],
            in_specs=[SMEM, VMEM if slot else HBM]
            + [VMEM] * (9 + len(sums))
            + [HBM] * len(stores),
            out_specs=[HBM] + [VMEM] * 8,
            input_output_aliases={11 + len(sums): 0} if stores else {},
            scratch_shapes=[
                pltpu.VMEM((width, columns), f32),
                pltpu.VMEM((width, 2 * columns), bf16),
                pltpu.VMEM((count, columns), f32),
                pltpu.SemaphoreType.DMA((BLOCKS + 1,)),
                *([] if slot else [pltpu.VMEM((width, width), f32)]),
            ],
            compiler_params=params(LATER if slot else 48),
            name="apply",
        )(scalars, matrix, pick, spread, local, *halo, *sums, *stores)
        return store, local, total, faces

    store, local, g1, faces = apply_call(0, block_inverse, local, halo)
    halo = exchange(faces, (4, 0, 5, 2, 3, 1))
    store, local, g2, faces = apply_call(1, local_schur, local, halo, (), (store,))
    halo = exchange(faces, (0, 4, 5, 2, 3, 1))
    store, local, g3, faces = apply_call(2, block_inverse, local, halo, (), (store,))
    halo = exchange(faces, (4, 5, 0, 1, 2, 3))
    store, local, sums, faces = apply_call(
        3, local_schur, local, halo, (g1, g2, g3), (store,)
    )
    sums = lax.all_to_all(sums, FIRST, 0, 0)
    sums = pl.pallas_call(
        relay_kernel,
        out_shape=shared[1],
        in_specs=[VMEM],
        out_specs=VMEM,
        compiler_params=params(16),
        name="relay",
    )(sums)
    sums = lax.all_to_all(sums, SECOND, 0, 0)
    halo = exchange(faces, (2, 4, 0, 3, 5, 1))
    solution, residual = pl.pallas_call(
        last_kernel,
        out_shape=[vector, vector],
        in_specs=[SMEM] + [VMEM] * 9 + [HBM],
        out_specs=[VMEM] * 2,
        scratch_shapes=[pltpu.VMEM((width, columns), f32)] * 4 + [pltpu.SemaphoreType.DMA((4,))],
        compiler_params=params(50),
        name="last",
    )(scalars, sums, spread, local, *halo, store)
    return (solution.reshape(1, 1, 1, width, columns), residual.reshape(1, 1, 1, width, columns))


def solution(mesh):
    gx, gy, gz = (mesh.shape[name] for name in ("gx", "gy", "gz"))
    split = Mesh(mesh.devices.reshape(gx, gy, gz // 2, 2), AXES)
    subdomain = P("gx", "gy", GZ)
    vectors = P("gx", "gy", GZ, None, None)
    return jax.shard_map(
        on_device,
        mesh=split,
        in_specs=(P(), P(), subdomain, P(), vectors),
        out_specs=(vectors, vectors),
        check_vma=False,
    )
```
